32 devices in a mesh: batch: 8 (over y, x, core), cols: 4 (over z).
Axes of the slice: x: 2, y: 2, z: 4, core: 2. Of those that a mesh axis runs over, the one named last changes fastest.
Arguments:
- grad_up: float32 [8, 1024, 4096], P('batch', None, 'cols'), may hold values from -0.875 to 0.875
- grad_down: float32 [8, 4096, 1024], P('batch', 'cols'), may hold values from -0.875 to 0.875
- grad_query: float32 [8, 1024, 1024], P('batch', None, 'cols'), may hold values from -0.875 to 0.875
- grad_key: float32 [8, 1024, 1024], P('batch', None, 'cols'), may hold values from -0.875 to 0.875
- grad_value: float32 [8, 1024, 1024], P('batch', None, 'cols'), may hold values from -0.875 to 0.875
- grad_mixed: float32 [8, 1024, 1024], P('batch', 'cols'), may hold values from -0.875 to 0.875
- grad_norm: float32 [8, 1024], P('batch'), may hold values from -8 to 8
- weight_up: float32 [1024, 4096], P('batch', 'cols'), may hold values from -0.1875 to 0.1875
- weight_down: float32 [4096, 1024], P('cols', 'batch'), may hold values from -0.09375 to 0.09375
- weight_query: float32 [1024, 1024], P('batch', 'cols'), may hold values from -0.1875 to 0.1875
- weight_key: float32 [1024, 1024], P('batch', 'cols'), may hold values from -0.1875 to 0.1875
- weight_value: float32 [1024, 1024], P('batch', 'cols'), may hold values from -0.1875 to 0.1875
- weight_mixed: float32 [1024, 1024], P('cols', 'batch'), may hold values from -0.1875 to 0.1875
- weight_norm: float32 [1024], P('batch'), may hold values from 0.25 to 1.75
- moment_up: float32 [1024, 4096], P('batch', 'cols'), may hold values from -1.75 to 1.75
- moment_down: float32 [4096, 1024], P('cols', 'batch'), may hold values from -1.75 to 1.75
- moment_query: float32 [1024, 1024], P('batch', 'cols'), may hold values from -1.75 to 1.75
- moment_key: float32 [1024, 1024], P('batch', 'cols'), may hold values from -1.75 to 1.75
- moment_value: float32 [1024, 1024], P('batch', 'cols'), may hold values from -1.75 to 1.75
- moment_mixed: float32 [1024, 1024], P('cols', 'batch'), may hold values from -1.75 to 1.75
- moment_norm: float32 [1024], P('batch'), may hold values from -1.75 to 1.75
Outputs:
- copy_up: bfloat16 [1024, 4096], P(None, 'cols')
- copy_down: bfloat16 [4096, 1024], P('cols')
- copy_query: bfloat16 [1024, 1024], P(None, 'cols')
- copy_key: bfloat16 [1024, 1024], P(None, 'cols')
- copy_value: bfloat16 [1024, 1024], P(None, 'cols')
- copy_mixed: bfloat16 [1024, 1024], P('cols')
- copy_norm: bfloat16 [1024], replicated
- new_up: float32 [1024, 4096], P('batch', 'cols')
- new_down: float32 [4096, 1024], P('cols', 'batch')
- new_query: float32 [1024, 1024], P('batch', 'cols')
- new_key: float32 [1024, 1024], P('batch', 'cols')
- new_value: float32 [1024, 1024], P('batch', 'cols')
- new_mixed: float32 [1024, 1024], P('cols', 'batch')
- new_norm: float32 [1024], P('batch')
- state_new_up: float32 [1024, 4096], P('batch', 'cols')
- state_new_down: float32 [4096, 1024], P('cols', 'batch')
- state_new_query: float32 [1024, 1024], P('batch', 'cols')
- state_new_key: float32 [1024, 1024], P('batch', 'cols')
- state_new_value: float32 [1024, 1024], P('batch', 'cols')
- state_new_mixed: float32 [1024, 1024], P('cols', 'batch')
- state_new_norm: float32 [1024], P('batch')
The draws below stay inside these ranges and needn't reach their ends.
All inputs are finite; a program needn't handle non-finite values.
Results may differ from the reference program's by a relative error of at most 0.008.
Values may be sent and summed in bfloat16 or wider, within the bound.
A program may use at most 64 MiB of HBM per device.

```python
import jax
import jax.numpy as jnp

WIDTH = 1024
INNER = 4096
ATTN = 1024
REPLICAS = 8


def spiked(entries, rng, source, target, blocks, factor):
    owner, partner = [(jnp.arange(entries.shape[dim]) // (entries.shape[dim] // blocks)).reshape([-1 if axis == dim else 1 for axis in range(entries.ndim)]) for dim in (source, target)]
    chosen = jax.random.permutation(rng, blocks)[partner]
    strong = (owner == chosen) | (owner == (partner + blocks // 2) % blocks)
    return jnp.where(strong, factor * entries, entries)


def steps_of(rng, dims, cuts, smallest, top_value):
    level = 1.0
    for dim, parts in cuts:
        heights = jax.random.uniform(jax.random.fold_in(jax.random.fold_in(rng, 6), dim), (parts,), jnp.float32, smallest / len(cuts), top_value / len(cuts))
        level = level * jnp.repeat(jnp.exp(heights), dims[dim] // parts).reshape((-1,) + (1,) * (len(dims) - 1 - dim))
    return level


def centred(key, shape, scale, bound, pieces=(), kind=jnp.bfloat16):
    loudness = steps_of(key, shape, pieces, -0.22, 0.18) if pieces else 1.0
    drawn = jax.random.normal(key, shape, jnp.float32) * scale * loudness
    return jnp.minimum(jnp.maximum(drawn, -bound), bound).astype(kind)


def bell_draw_with(own_key, shape, deviation, most, split, heavy, kind=jnp.bfloat16):
    array = deviation * jax.random.normal(own_key, shape, jnp.float32)
    if split:
        array = array * steps_of(own_key, shape, split, -0.22, 0.18)
    return jnp.clip(spiked(array, jax.random.fold_in(own_key, 3), *heavy), -most, most).astype(kind)


def setup_inputs(seed: int = 0) -> dict:
    arg_keys = jax.random.split(jax.random.key(seed), 22)
    return {
        "grad_up": bell_draw_with(arg_keys[0], (REPLICAS, WIDTH, INNER), 0.1, 0.875, ((0, 8), (2, 4)), (0, 1, 8, 2.0), jnp.float32),
        "grad_down": bell_draw_with(arg_keys[1], (REPLICAS, INNER, WIDTH), 0.1, 0.875, ((0, 8), (1, 4)), (0, 2, 8, 2.0), jnp.float32),
        "grad_query": bell_draw_with(arg_keys[2], (REPLICAS, WIDTH, ATTN), 0.1, 0.875, ((0, 8), (2, 4)), (0, 1, 8, 2.0), jnp.float32),
        "grad_key": bell_draw_with(arg_keys[3], (REPLICAS, WIDTH, ATTN), 0.1, 0.875, ((0, 8), (2, 4)), (0, 1, 8, 2.0), jnp.float32),
        "grad_value": bell_draw_with(arg_keys[4], (REPLICAS, WIDTH, ATTN), 0.1, 0.875, ((0, 8), (2, 4)), (0, 1, 8, 2.0), jnp.float32),
        "grad_mixed": bell_draw_with(arg_keys[5], (REPLICAS, ATTN, WIDTH), 0.1, 0.875, ((0, 8), (1, 4)), (0, 2, 8, 2.0), jnp.float32),
        "grad_norm": bell_draw_with(arg_keys[6], (REPLICAS, WIDTH), 1.0, 8.0, ((0, 8),), (0, 1, 8, 2.0), jnp.float32),
        "weight_up": centred(arg_keys[7], (WIDTH, INNER), WIDTH ** -0.5, 0.1875, ((0, 8), (1, 4)), jnp.float32),
        "weight_down": centred(arg_keys[8], (INNER, WIDTH), INNER ** -0.5, 0.09375, ((0, 4), (1, 8)), jnp.float32),
        "weight_query": centred(arg_keys[9], (WIDTH, ATTN), WIDTH ** -0.5, 0.1875, ((0, 8), (1, 4)), jnp.float32),
        "weight_key": centred(arg_keys[10], (WIDTH, ATTN), WIDTH ** -0.5, 0.1875, ((0, 8), (1, 4)), jnp.float32),
        "weight_value": centred(arg_keys[11], (WIDTH, ATTN), WIDTH ** -0.5, 0.1875, ((0, 8), (1, 4)), jnp.float32),
        "weight_mixed": centred(arg_keys[12], (ATTN, WIDTH), ATTN ** -0.5, 0.1875, ((0, 4), (1, 8)), jnp.float32),
        "weight_norm": jnp.clip(1.0 + 0.15 * jax.random.normal(arg_keys[13], (WIDTH,), jnp.float32), 0.25, 1.75),
        "moment_up": centred(arg_keys[14], (WIDTH, INNER), 0.3, 1.75, ((0, 8), (1, 4)), jnp.float32),
        "moment_down": centred(arg_keys[15], (INNER, WIDTH), 0.3, 1.75, ((0, 4), (1, 8)), jnp.float32),
        "moment_query": centred(arg_keys[16], (WIDTH, ATTN), 0.3, 1.75, ((0, 8), (1, 4)), jnp.float32),
        "moment_key": centred(arg_keys[17], (WIDTH, ATTN), 0.3, 1.75, ((0, 8), (1, 4)), jnp.float32),
        "moment_value": centred(arg_keys[18], (WIDTH, ATTN), 0.3, 1.75, ((0, 8), (1, 4)), jnp.float32),
        "moment_mixed": centred(arg_keys[19], (ATTN, WIDTH), 0.3, 1.75, ((0, 4), (1, 8)), jnp.float32),
        "moment_norm": centred(arg_keys[20], (WIDTH,), 0.3, 1.75, ((0, 8),), jnp.float32),
    }


learn_rate = 0.1
hold_rate = 0.7


def reference(grad_up, grad_down, grad_query, grad_key, grad_value, grad_mixed, grad_norm, weight_up, weight_down, weight_query, weight_key, weight_value, weight_mixed, weight_norm, moment_up, moment_down, moment_query, moment_key, moment_value, moment_mixed, moment_norm):
    mean_up = jnp.sum(grad_up.astype(jnp.float32), axis=0) * REPLICAS ** -0.5
    mean_down = jnp.sum(grad_down.astype(jnp.float32), axis=0) * REPLICAS ** -0.5
    mean_query = jnp.sum(grad_query.astype(jnp.float32), axis=0) * REPLICAS ** -0.5
    mean_key = jnp.sum(grad_key.astype(jnp.float32), axis=0) * REPLICAS ** -0.5
    mean_value = jnp.sum(grad_value.astype(jnp.float32), axis=0) * REPLICAS ** -0.5
    mean_mixed = jnp.sum(grad_mixed.astype(jnp.float32), axis=0) * REPLICAS ** -0.5
    mean_norm = jnp.sum(grad_norm.astype(jnp.float32), axis=0) * REPLICAS ** -0.5
    state_new_up = hold_rate * moment_up + mean_up
    new_up = weight_up - learn_rate * state_new_up
    state_new_down = hold_rate * moment_down + mean_down
    new_down = weight_down - learn_rate * state_new_down
    state_new_query = hold_rate * moment_query + mean_query
    new_query = weight_query - learn_rate * state_new_query
    state_new_key = hold_rate * moment_key + mean_key
    new_key = weight_key - learn_rate * state_new_key
    state_new_value = hold_rate * moment_value + mean_value
    new_value = weight_value - learn_rate * state_new_value
    state_new_mixed = hold_rate * moment_mixed + mean_mixed
    new_mixed = weight_mixed - learn_rate * state_new_mixed
    state_new_norm = hold_rate * moment_norm + mean_norm
    new_norm = weight_norm - learn_rate * state_new_norm
    copy_up = new_up.astype(jnp.bfloat16)
    copy_down = new_down.astype(jnp.bfloat16)
    copy_query = new_query.astype(jnp.bfloat16)
    copy_key = new_key.astype(jnp.bfloat16)
    copy_value = new_value.astype(jnp.bfloat16)
    copy_mixed = new_mixed.astype(jnp.bfloat16)
    copy_norm = new_norm.astype(jnp.bfloat16)
    return copy_up, copy_down, copy_query, copy_key, copy_value, copy_mixed, copy_norm, new_up, new_down, new_query, new_key, new_value, new_mixed, new_norm, state_new_up, state_new_down, state_new_query, state_new_key, state_new_value, state_new_mixed, state_new_norm
```

```python
import functools

import jax
import jax.numpy as jnp
from jax import lax
from jax.experimental import pallas as pl
from jax.experimental.pallas import tpu as pltpu
from jax.sharding import PartitionSpec as P

learn_rate = 0.1
hold_rate = 0.7


def body(
    grad_up,
    grad_down,
    grad_query,
    grad_key,
    grad_value,
    grad_mixed,
    grad_norm,
    weight_up,
    weight_down,
    weight_query,
    weight_key,
    weight_value,
    weight_mixed,
    weight_norm,
    moment_up,
    moment_down,
    moment_query,
    moment_key,
    moment_value,
    moment_mixed,
    moment_norm,
):
    mean_up, mean_down, mean_query, mean_key, mean_value, mean_mixed = (
        lax.psum_scatter(
            grad_up[0].astype(jnp.bfloat16), "batch", scatter_dimension=0, tiled=True
        ).astype(jnp.float32),
        lax.psum_scatter(
            grad_down[0].astype(jnp.bfloat16), "batch", scatter_dimension=1, tiled=True
        ).astype(jnp.float32),
        lax.psum_scatter(
            grad_query[0].astype(jnp.bfloat16), "batch", scatter_dimension=0, tiled=True
        ).astype(jnp.float32),
        lax.psum_scatter(
            grad_key[0].astype(jnp.bfloat16), "batch", scatter_dimension=0, tiled=True
        ).astype(jnp.float32),
        lax.psum_scatter(
            grad_value[0].astype(jnp.bfloat16), "batch", scatter_dimension=0, tiled=True
        ).astype(jnp.float32),
        lax.psum_scatter(
            grad_mixed[0].astype(jnp.bfloat16), "batch", scatter_dimension=1, tiled=True
        ).astype(jnp.float32),
    )
    whole_norm = lax.psum(grad_norm[0], "batch")
    place = lax.axis_index("batch")
    mean_norm = lax.dynamic_slice_in_dim(
        whole_norm, place * weight_norm.shape[0], weight_norm.shape[0]
    )
    mean_rate = lax.axis_size("batch") ** (-0.5)
    mean_up = mean_up * mean_rate
    mean_down = mean_down * mean_rate
    mean_query = mean_query * mean_rate
    mean_key = mean_key * mean_rate
    mean_value = mean_value * mean_rate
    mean_mixed = mean_mixed * mean_rate
    mean_norm = mean_norm * mean_rate
    state_new_up = hold_rate * moment_up + mean_up
    new_up = weight_up - learn_rate * state_new_up
    state_new_down = hold_rate * moment_down + mean_down
    new_down = weight_down - learn_rate * state_new_down
    state_new_query = hold_rate * moment_query + mean_query
    new_query = weight_query - learn_rate * state_new_query
    state_new_key = hold_rate * moment_key + mean_key
    new_key = weight_key - learn_rate * state_new_key
    state_new_value = hold_rate * moment_value + mean_value
    new_value = weight_value - learn_rate * state_new_value
    state_new_mixed = hold_rate * moment_mixed + mean_mixed
    new_mixed = weight_mixed - learn_rate * state_new_mixed
    state_new_norm = hold_rate * moment_norm + mean_norm
    new_norm = weight_norm - learn_rate * state_new_norm
    copy_up, copy_down, copy_query, copy_key, copy_value, copy_mixed, copy_norm = (
        lax.all_gather(new_up.astype(jnp.bfloat16), "batch", axis=0, tiled=True),
        lax.all_gather(new_down.astype(jnp.bfloat16), "batch", axis=1, tiled=True),
        lax.all_gather(new_query.astype(jnp.bfloat16), "batch", axis=0, tiled=True),
        lax.all_gather(new_key.astype(jnp.bfloat16), "batch", axis=0, tiled=True),
        lax.all_gather(new_value.astype(jnp.bfloat16), "batch", axis=0, tiled=True),
        lax.all_gather(new_mixed.astype(jnp.bfloat16), "batch", axis=1, tiled=True),
        lax.all_gather(new_norm.astype(jnp.bfloat16), "batch", axis=0, tiled=True),
    )
    return (
        copy_up,
        copy_down,
        copy_query,
        copy_key,
        copy_value,
        copy_mixed,
        copy_norm,
        new_up,
        new_down,
        new_query,
        new_key,
        new_value,
        new_mixed,
        new_norm,
        state_new_up,
        state_new_down,
        state_new_query,
        state_new_key,
        state_new_value,
        state_new_mixed,
        state_new_norm,
    )


PIECES = (4, 4, 1, 1, 1, 1)
X_FIRST = (0, 2, 3)
Y_FIRST = (1, 5, 4)
BY_ROWS = (True, False, True, True, True, False)
LOAD, SEND, RECV, OWN, NEW, STATE, KINDS = 0, 1, 7, 13, 14, 15, 16


def pieces_of(shapes):
    lists = []
    for names, x_first in ((X_FIRST, True), (Y_FIRST, False)):
        lists.append([])
        for m in names:
            rows = shapes[m][0] // PIECES[m]
            for k in range(PIECES[m]):
                lists[-1].append((m, k, rows, x_first))
    return lists


def exchange(shapes, n, *refs):
    refs = list(refs)

    def take(count):
        out, refs[:] = refs[:count], refs[count:]
        return out

    grads, weights, moments = take(6), take(6), take(6)
    grad_norm, weight_norm, moment_norm = take(3)
    gathered, news, states = take(6), take(6), take(6)
    norm_pack, norm_out = take(2)
    grad_v, weight_v, moment_v, new_v, state_v = (take(6) for _ in range(5))
    send_1, recv_1, send_2, recv_2, keep_2 = (take(6) for _ in range(5))
    send_3, recv_3, keep_3, own_v = (take(6) for _ in range(4))
    norm_send, norm_recv, norm_all = take(3)
    sems, param_sems, norm_sems, norm_sems_2 = take(4)

    me = lax.axis_index("batch")
    c = lax.rem(me, 2)
    x = lax.rem(lax.div(me, 2), 2)
    y = lax.div(me, 4)
    other_c, other_x, other_y = me + 1 - 2 * c, me + 2 - 4 * x, me + 4 - 8 * y
    rate = n ** (-0.5)

    lists = pieces_of(shapes)
    pairs = len(lists[0])
    number = {}
    for p in range(pairs):
        for s in range(2):
            number[lists[s][p][:2]] = 2 * p + s

    def sem(piece, kind):
        return sems.at[number[piece[:2]], kind]

    def load(piece):
        m, k, rows, _ = piece
        at = pl.ds(k * rows, rows)
        if BY_ROWS[m]:
            source, target = grads[m].at[:, at, :], grad_v[m].at[:, at, :]
        else:
            source, target = grads[m].at[at, :], grad_v[m].at[at, :]
        return pltpu.make_async_copy(source, target, sem(piece, LOAD))

    def params(m):
        return (
            pltpu.make_async_copy(weights[m], weight_v[m], param_sems.at[m, 0]),
            pltpu.make_async_copy(moments[m], moment_v[m], param_sems.at[m, 1]),
        )

    def remote(piece, step, source, target, device):
        return pltpu.make_async_remote_copy(
            src_ref=source,
            dst_ref=target,
            send_sem=sem(piece, SEND + step),
            recv_sem=sem(piece, RECV + step),
            device_id={"batch": device},
            device_id_type=pl.DeviceIdType.MESH,
        )

    def hop(piece, step):
        m, k, rows, x_first = piece
        first, second = (other_x, other_y) if x_first else (other_y, other_x)
        place = gathered[m]
        if step == 0:
            return remote(piece, 0, send_1[m].at[k], recv_1[m].at[k], other_c)
        if step == 1:
            return remote(piece, 1, send_2[m].at[k], recv_2[m].at[k], first)
        if step == 2:
            return remote(piece, 2, send_3[m].at[k], recv_3[m].at[k], second)
        if step == 3:
            return remote(piece, 3, own_v[m].at[k], place.at[k, y, x, c], second)
        if step == 4:
            part = place.at[k, :, x, c] if x_first else place.at[k, y, :, c]
            return remote(piece, 4, part, part, first)
        part = place.at[k, :, :, c]
        return remote(piece, 5, part, part, other_c)

    def own_copies(piece):
        m, k, rows, _ = piece
        at = pl.ds(k * rows, rows)
        return (
            pltpu.make_async_copy(own_v[m].at[k], gathered[m].at[k, y, x, c], sem(piece, OWN)),
            pltpu.make_async_copy(new_v[m].at[at, :], news[m].at[at, :], sem(piece, NEW)),
            pltpu.make_async_copy(state_v[m].at[at, :], states[m].at[at, :], sem(piece, STATE)),
        )

    def block(piece, owner):
        m, k, rows, _ = piece
        at = pl.ds(k * rows, rows)
        if BY_ROWS[m]:
            return grad_v[m][owner, at, :]
        width = shapes[m][1]
        return grad_v[m][at, pl.ds(pl.multiple_of(owner * width, width), width)]

    def stage(piece, step):
        m, k, rows, x_first = piece
        f, s = (x, y) if x_first else (y, x)

        def spot(first, second):
            return 2 * second + first if x_first else 2 * first + second

        if step == 0:
            load(piece).wait()
            for q in range(4):
                send_1[m][k, q] = block(piece, 2 * q + 1 - c).astype(jnp.bfloat16)
            hop(piece, 0).start()
        elif step == 1:
            hop(piece, 0).wait_recv()
            for second in range(2):
                q = spot(1 - f, second)
                total = block(piece, 2 * q + c) + recv_1[m][k, q].astype(jnp.float32)
                send_2[m][k, second] = total.astype(jnp.bfloat16)
            hop(piece, 1).start()
            for second in range(2):
                q = spot(f, second)
                keep_2[m][k, second] = block(piece, 2 * q + c) + recv_1[m][k, q].astype(jnp.float32)
        elif step == 2:
            hop(piece, 1).wait_recv()
            total = keep_2[m][k, 1 - s] + recv_2[m][k, 1 - s].astype(jnp.float32)
            send_3[m][k] = total.astype(jnp.bfloat16)
            hop(piece, 2).start()
            keep_3[m][k] = keep_2[m][k, s] + recv_2[m][k, s].astype(jnp.float32)
        elif step == 3:
            if k == 0:
                for copy in params(m):
                    copy.wait()
            hop(piece, 2).wait_recv()
            at = pl.ds(k * rows, rows)
            mean = (keep_3[m][k] + recv_3[m][k].astype(jnp.float32)) * rate
            state = hold_rate * moment_v[m][at, :] + mean
            new = weight_v[m][at, :] - learn_rate * state
            own_v[m][k] = new.astype(jnp.bfloat16)
            hop(piece, 3).start()
            new_v[m][at, :] = new
            state_v[m][at, :] = state
            for copy in own_copies(piece):
                copy.start()
        elif step == 4:
            own_copies(piece)[0].wait()
            hop(piece, 3).wait_recv()
            hop(piece, 4).start()
        elif step == 5:
            hop(piece, 4).wait_recv()
            hop(piece, 5).start()
        else:
            hop(piece, 5).wait_recv()

    started = set()
    for p in range(pairs):
        for s in range(2):
            load(lists[s][p]).start()
        if p >= 1:
            for s in range(2):
                m = lists[s][p - 1][0]
                if m not in started:
                    started.add(m)
                    for copy in params(m):
                        copy.start()
    for m in range(6):
        if m not in started:
            for copy in params(m):
                copy.start()

    barrier = pltpu.get_barrier_semaphore()
    for d in range(1, n):
        pl.semaphore_signal(
            barrier, inc=1, device_id={"batch": lax.rem(me + d, n)}, device_id_type=pl.DeviceIdType.MESH
        )
    pl.semaphore_wait(barrier, n - 1)

    width = weight_norm.shape[1]

    def norm_hop(d):
        to = lax.rem(me + d, n)
        return pltpu.make_async_remote_copy(
            src_ref=norm_send.at[to],
            dst_ref=norm_recv.at[d],
            send_sem=norm_sems.at[0, d],
            recv_sem=norm_sems.at[1, d],
            device_id={"batch": to},
            device_id_type=pl.DeviceIdType.MESH,
        )

    def norm_back(d):
        to = lax.rem(me + d, n)
        return pltpu.make_async_remote_copy(
            src_ref=norm_pack.at[0],
            dst_ref=norm_all.at[d],
            send_sem=norm_sems_2.at[0, d],
            recv_sem=norm_sems_2.at[1, d],
            device_id={"batch": to},
            device_id_type=pl.DeviceIdType.MESH,
        )

    def norm_start():
        for j in range(n):
            part = grad_norm[:, j * width : (j + 1) * width]
            norm_send[j] = jnp.broadcast_to(part, (8, width))
        for d in range(1, n):
            norm_hop(d).start()

    def norm_update():
        total = norm_send[me]
        for d in range(1, n):
            norm_hop(d).wait_recv()
            total = total + norm_recv[d]
        state = hold_rate * moment_norm[...] + total * rate
        norm_pack[1] = state
        norm_pack[0] = weight_norm[...] - learn_rate * state
        for d in range(1, n):
            norm_back(d).start()

    def norm_end():
        norm_out[me] = norm_pack[0]
        for d in range(1, n):
            norm_back(d).wait_recv()
            norm_out[lax.rem(me + n - d, n)] = norm_all[d]

    for slot in range(pairs + 6):
        for step in range(6, -1, -1):
            p = slot - step
            if 0 <= p < pairs:
                for s in range(2):
                    stage(lists[s][p], step)
        if slot == 1:
            norm_start()
        if slot == 3:
            norm_update()
    norm_end()

    for p in range(pairs):
        for s in range(2):
            piece = lists[s][p]
            for step in range(6):
                hop(piece, step).wait_send()
            for copy in own_copies(piece)[1:]:
                copy.wait()
    for d in range(1, n):
        norm_hop(d).wait_send()
        norm_back(d).wait_send()


def write_out(shapes, n, *refs):
    refs = list(refs)

    def take(count):
        out, refs[:] = refs[:count], refs[count:]
        return out

    gathered, news, states = take(6), take(6), take(6)
    norm_pack, norm_out = take(2)
    copies, new_outs, state_outs = take(6), take(6), take(6)
    copy_norm, new_norm, state_norm = take(3)
    (sems,) = take(1)
    started = []
    count = 0
    for m in range(6):
        rows = shapes[m][0] // PIECES[m]
        width = shapes[m][1]
        for k in range(PIECES[m]):
            for j in range(n):
                source = gathered[m].at[k, j // 4, j // 2 % 2, j % 2]
                if BY_ROWS[m]:
                    target = copies[m].at[pl.ds(j * shapes[m][0] + k * rows, rows), :]
                else:
                    target = copies[m].at[pl.ds(k * rows, rows), pl.ds(j * width, width)]
                started.append(pltpu.make_async_copy(source, target, sems.at[count]))
                count += 1
        for source, target in ((news[m], new_outs[m]), (states[m], state_outs[m])):
            started.append(pltpu.make_async_copy(source, target, sems.at[count]))
            count += 1
    for copy in started:
        copy.start()
    for j in range(n):
        width = norm_out.shape[2]
        copy_norm[:, j * width : (j + 1) * width] = norm_out[j, 0:1, :].astype(jnp.bfloat16)
    new_norm[...] = norm_pack[0, 0:1, :]
    state_norm[...] = norm_pack[1, 0:1, :]
    for copy in started:
        copy.wait()


def kernel_body(*args):
    n = lax.axis_size("batch")
    grads, grad_norm = [a[0] for a in args[:6]], args[6]
    weights, weight_norm = args[7:13], args[13]
    moments, moment_norm = args[14:20], args[20]
    shapes = [w.shape for w in weights]
    grads = [g.reshape((n, *s)) if by_rows else g for g, s, by_rows in zip(grads, shapes, BY_ROWS)]
    width = weight_norm.shape[0]
    bf16, f32 = jnp.bfloat16, jnp.float32
    any_spec = pl.BlockSpec(memory_space=pl.ANY)
    vmem_spec = pl.BlockSpec(memory_space=pltpu.VMEM)
    hbm_spec = pl.BlockSpec(memory_space=pltpu.HBM)

    def cut(m):
        rows, cols = shapes[m]
        return PIECES[m], rows // PIECES[m], cols

    every = range(6)

    def scratch(lead, kind):
        return [pltpu.VMEM((cut(m)[0], *lead, *cut(m)[1:]), kind) for m in every]

    whole = [pltpu.VMEM(s, f32) for s in shapes]
    held = [pltpu.VMEM((cut(m)[0], 2, 2, 2, *cut(m)[1:]), bf16) for m in every] + whole + whole
    lists = pieces_of(shapes)
    assert len(lists[0]) == len(lists[1])
    results = pl.pallas_call(
        functools.partial(exchange, shapes, n),
        out_shape=held
        + [jax.ShapeDtypeStruct((2, 8, width), f32), jax.ShapeDtypeStruct((n, 8, width), f32)],
        in_specs=[any_spec] * 18 + [vmem_spec] * 3,
        out_specs=[any_spec] * 18 + [vmem_spec] * 2,
        scratch_shapes=[pltpu.VMEM(g.shape, f32) for g in grads]
        + whole * 4
        + scratch((4,), bf16) * 2
        + scratch((2,), bf16) * 2
        + scratch((2,), f32)
        + scratch((), bf16) * 2
        + scratch((), f32)
        + scratch((), bf16)
        + [pltpu.VMEM((n, 8, width), f32)] * 3
        + [
            pltpu.SemaphoreType.DMA((2 * len(lists[0]), KINDS)),
            pltpu.SemaphoreType.DMA((6, 2)),
            pltpu.SemaphoreType.DMA((2, n)),
            pltpu.SemaphoreType.DMA((2, n)),
        ],
        compiler_params=pltpu.CompilerParams(
            collective_id=0, has_side_effects=True, vmem_limit_bytes=40 * 2**20
        ),
    )(*grads, *weights, *moments, grad_norm, weight_norm.reshape(1, width), moment_norm.reshape(1, width))
    copies = n * sum(PIECES) + 12
    finals = pl.pallas_call(
        functools.partial(write_out, shapes, n),
        out_shape=[
            jax.ShapeDtypeStruct((n * s[0], s[1]) if by_rows else (s[0], n * s[1]), bf16)
            for s, by_rows in zip(shapes, BY_ROWS)
        ]
        + [jax.ShapeDtypeStruct(s, f32) for s in shapes] * 2
        + [
            jax.ShapeDtypeStruct((1, n * width), bf16),
            jax.ShapeDtypeStruct((1, width), f32),
            jax.ShapeDtypeStruct((1, width), f32),
        ],
        in_specs=[any_spec] * 18 + [vmem_spec] * 2,
        out_specs=[hbm_spec] * 18 + [vmem_spec] * 3,
        scratch_shapes=[pltpu.SemaphoreType.DMA((copies,))],
        compiler_params=pltpu.CompilerParams(vmem_limit_bytes=8 * 2**20),
    )(*[pltpu.with_memory_space_constraint(r, pltpu.VMEM) for r in results[:18]], *results[18:])
    copy, new, state = finals[:6], finals[6:12], finals[12:18]
    copy_norm, new_norm, state_norm = (r.reshape(r.shape[1]) for r in finals[18:])
    return (*copy, copy_norm, *new, new_norm, *state, state_norm)


def chosen(*args):
    fits = lax.axis_size("batch") == 2**3 and args[13].shape[0] % 128 == 0
    for w, count in zip(args[7:13], PIECES):
        fits = fits and w.shape[0] % (16 * count) == 0 and w.shape[1] % 128 == 0
    return kernel_body(*args) if fits else body(*args)


def solution(mesh):
    in_specs = (
        P("batch", None, "cols"),
        P("batch", "cols", None),
        P("batch", None, "cols"),
        P("batch", None, "cols"),
        P("batch", None, "cols"),
        P("batch", "cols", None),
        P("batch", None),
        P("batch", "cols"),
        P("cols", "batch"),
        P("batch", "cols"),
        P("batch", "cols"),
        P("batch", "cols"),
        P("cols", "batch"),
        P("batch"),
        P("batch", "cols"),
        P("cols", "batch"),
        P("batch", "cols"),
        P("batch", "cols"),
        P("batch", "cols"),
        P("cols", "batch"),
        P("batch"),
    )
    out_specs = (
        P(None, "cols"),
        P("cols", None),
        P(None, "cols"),
        P(None, "cols"),
        P(None, "cols"),
        P("cols", None),
        P(),
        P("batch", "cols"),
        P("cols", "batch"),
        P("batch", "cols"),
        P("batch", "cols"),
        P("batch", "cols"),
        P("cols", "batch"),
        P("batch"),
        P("batch", "cols"),
        P("cols", "batch"),
        P("batch", "cols"),
        P("batch", "cols"),
        P("batch", "cols"),
        P("cols", "batch"),
        P("batch"),
    )
    return jax.shard_map(chosen, mesh=mesh, in_specs=in_specs, out_specs=out_specs, check_vma=False)
```

```python
import functools

import jax
import jax.numpy as jnp
from jax import lax
from jax.experimental import pallas as pl
from jax.experimental.pallas import tpu as pltpu
from jax.sharding import PartitionSpec as P

learn_rate = 0.1
hold_rate = 0.7


def body(
    grad_up,
    grad_down,
    grad_query,
    grad_key,
    grad_value,
    grad_mixed,
    grad_norm,
    weight_up,
    weight_down,
    weight_query,
    weight_key,
    weight_value,
    weight_mixed,
    weight_norm,
    moment_up,
    moment_down,
    moment_query,
    moment_key,
    moment_value,
    moment_mixed,
    moment_norm,
):
    mean_up, mean_down, mean_query, mean_key, mean_value, mean_mixed = (
        lax.psum_scatter(
            grad_up[0].astype(jnp.bfloat16), "batch", scatter_dimension=0, tiled=True
        ).astype(jnp.float32),
        lax.psum_scatter(
            grad_down[0].astype(jnp.bfloat16), "batch", scatter_dimension=1, tiled=True
        ).astype(jnp.float32),
        lax.psum_scatter(
            grad_query[0].astype(jnp.bfloat16), "batch", scatter_dimension=0, tiled=True
        ).astype(jnp.float32),
        lax.psum_scatter(
            grad_key[0].astype(jnp.bfloat16), "batch", scatter_dimension=0, tiled=True
        ).astype(jnp.float32),
        lax.psum_scatter(
            grad_value[0].astype(jnp.bfloat16), "batch", scatter_dimension=0, tiled=True
        ).astype(jnp.float32),
        lax.psum_scatter(
            grad_mixed[0].astype(jnp.bfloat16), "batch", scatter_dimension=1, tiled=True
        ).astype(jnp.float32),
    )
    whole_norm = lax.psum(grad_norm[0], "batch")
    place = lax.axis_index("batch")
    mean_norm = lax.dynamic_slice_in_dim(
        whole_norm, place * weight_norm.shape[0], weight_norm.shape[0]
    )
    mean_rate = lax.axis_size("batch") ** (-0.5)
    mean_up = mean_up * mean_rate
    mean_down = mean_down * mean_rate
    mean_query = mean_query * mean_rate
    mean_key = mean_key * mean_rate
    mean_value = mean_value * mean_rate
    mean_mixed = mean_mixed * mean_rate
    mean_norm = mean_norm * mean_rate
    state_new_up = hold_rate * moment_up + mean_up
    new_up = weight_up - learn_rate * state_new_up
    state_new_down = hold_rate * moment_down + mean_down
    new_down = weight_down - learn_rate * state_new_down
    state_new_query = hold_rate * moment_query + mean_query
    new_query = weight_query - learn_rate * state_new_query
    state_new_key = hold_rate * moment_key + mean_key
    new_key = weight_key - learn_rate * state_new_key
    state_new_value = hold_rate * moment_value + mean_value
    new_value = weight_value - learn_rate * state_new_value
    state_new_mixed = hold_rate * moment_mixed + mean_mixed
    new_mixed = weight_mixed - learn_rate * state_new_mixed
    state_new_norm = hold_rate * moment_norm + mean_norm
    new_norm = weight_norm - learn_rate * state_new_norm
    copy_up, copy_down, copy_query, copy_key, copy_value, copy_mixed, copy_norm = (
        lax.all_gather(new_up.astype(jnp.bfloat16), "batch", axis=0, tiled=True),
        lax.all_gather(new_down.astype(jnp.bfloat16), "batch", axis=1, tiled=True),
        lax.all_gather(new_query.astype(jnp.bfloat16), "batch", axis=0, tiled=True),
        lax.all_gather(new_key.astype(jnp.bfloat16), "batch", axis=0, tiled=True),
        lax.all_gather(new_value.astype(jnp.bfloat16), "batch", axis=0, tiled=True),
        lax.all_gather(new_mixed.astype(jnp.bfloat16), "batch", axis=1, tiled=True),
        lax.all_gather(new_norm.astype(jnp.bfloat16), "batch", axis=0, tiled=True),
    )
    return (
        copy_up,
        copy_down,
        copy_query,
        copy_key,
        copy_value,
        copy_mixed,
        copy_norm,
        new_up,
        new_down,
        new_query,
        new_key,
        new_value,
        new_mixed,
        new_norm,
        state_new_up,
        state_new_down,
        state_new_query,
        state_new_key,
        state_new_value,
        state_new_mixed,
        state_new_norm,
    )


PIECES = (4, 4, 1, 1, 1, 1)
DELAYS = (0, 1, 2, 3, 4, 5, 6)
STEP_ORDER = (0, 1, 2, 3, 4, 5, 6)
X_FIRST = (0, 2, 3)
Y_FIRST = (1, 5, 4)
BY_ROWS = (True, False, True, True, True, False)
LOAD, SEND, RECV, OWN, NEW, STATE, KINDS = 0, 1, 7, 13, 14, 15, 16


def pieces_of(shapes):
    lists = []
    for names, x_first in ((X_FIRST, True), (Y_FIRST, False)):
        lists.append([])
        for m in names:
            rows = shapes[m][0] // PIECES[m]
            for k in range(PIECES[m]):
                lists[-1].append((m, k, rows, x_first))
    return lists


def exchange(shapes, n, *refs):
    refs = list(refs)

    def take(count):
        out, refs[:] = refs[:count], refs[count:]
        return out

    grads, weights, moments = take(6), take(6), take(6)
    norm_inputs = take(3)
    gathered, news, states = take(6), take(6), take(6)
    norm_pack, norm_out = take(2)
    grad_v, weight_v, moment_v, new_v, state_v = (take(6) for _ in range(5))
    send_1, recv_1, send_2, recv_2, keep_2 = (take(6) for _ in range(5))
    send_3, recv_3, keep_3, own_v = (take(6) for _ in range(4))
    norm_send, norm_recv, norm_all = take(3)
    norm_held = take(3)
    grad_norm, weight_norm, moment_norm = norm_held
    sems, param_sems, norm_sems, norm_sems_2, norm_sems_3 = take(5)

    me = lax.axis_index("batch")
    c = lax.rem(me, 2)
    x = lax.rem(lax.div(me, 2), 2)
    y = lax.div(me, 4)
    other_c, other_x, other_y = me + 1 - 2 * c, me + 2 - 4 * x, me + 4 - 8 * y
    rate = n ** (-0.5)

    lists = pieces_of(shapes)
    pairs = len(lists[0])
    number = {}
    for p in range(pairs):
        for s in range(2):
            number[lists[s][p][:2]] = 2 * p + s

    def sem(piece, kind):
        return sems.at[number[piece[:2]], kind]

    def load(piece):
        m, k, rows, _ = piece
        at = pl.ds(k * rows, rows)
        if BY_ROWS[m]:
            source, target = grads[m].at[:, at, :], grad_v[m].at[:, at, :]
        else:
            source, target = grads[m].at[at, :], grad_v[m].at[at, :]
        return pltpu.make_async_copy(source, target, sem(piece, LOAD))

    def params(m):
        return (
            pltpu.make_async_copy(weights[m], weight_v[m], param_sems.at[m, 0]),
            pltpu.make_async_copy(moments[m], moment_v[m], param_sems.at[m, 1]),
        )

    def remote(piece, step, source, target, device):
        return pltpu.make_async_remote_copy(
            src_ref=source,
            dst_ref=target,
            send_sem=sem(piece, SEND + step),
            recv_sem=sem(piece, RECV + step),
            device_id={"batch": device},
            device_id_type=pl.DeviceIdType.MESH,
        )

    def hop(piece, step):
        m, k, rows, x_first = piece
        first, second = (other_x, other_y) if x_first else (other_y, other_x)
        place = gathered[m]
        if step == 0:
            return remote(piece, 0, send_1[m].at[k], recv_1[m].at[k], other_c)
        if step == 1:
            return remote(piece, 1, send_2[m].at[k], recv_2[m].at[k], first)
        if step == 2:
            return remote(piece, 2, send_3[m].at[k], recv_3[m].at[k], second)
        if step == 3:
            return remote(piece, 3, own_v[m].at[k], place.at[k, y, x, c], second)
        if step == 4:
            part = place.at[k, :, x, c] if x_first else place.at[k, y, :, c]
            return remote(piece, 4, part, part, first)
        part = place.at[k, :, :, c]
        return remote(piece, 5, part, part, other_c)

    def own_copies(piece):
        m, k, rows, _ = piece
        at = pl.ds(k * rows, rows)
        return (
            pltpu.make_async_copy(own_v[m].at[k], gathered[m].at[k, y, x, c], sem(piece, OWN)),
            pltpu.make_async_copy(new_v[m].at[at, :], news[m].at[at, :], sem(piece, NEW)),
            pltpu.make_async_copy(state_v[m].at[at, :], states[m].at[at, :], sem(piece, STATE)),
        )

    def block(piece, owner):
        m, k, rows, _ = piece
        at = pl.ds(k * rows, rows)
        if BY_ROWS[m]:
            return grad_v[m][owner, at, :]
        width = shapes[m][1]
        return grad_v[m][at, pl.ds(pl.multiple_of(owner * width, width), width)]

    def stage(piece, step):
        m, k, rows, x_first = piece
        f, s = (x, y) if x_first else (y, x)

        def spot(first, second):
            return 2 * second + first if x_first else 2 * first + second

        if step == 0:
            load(piece).wait()
            for q in range(4):
                send_1[m][k, q] = block(piece, 2 * q + 1 - c).astype(jnp.bfloat16)
            hop(piece, 0).start()
        elif step == 1:
            hop(piece, 0).wait_recv()
            for second in range(2):
                q = spot(1 - f, second)
                total = block(piece, 2 * q + c) + recv_1[m][k, q].astype(jnp.float32)
                send_2[m][k, second] = total.astype(jnp.bfloat16)
            hop(piece, 1).start()
            for second in range(2):
                q = spot(f, second)
                keep_2[m][k, second] = block(piece, 2 * q + c) + recv_1[m][k, q].astype(jnp.float32)
        elif step == 2:
            hop(piece, 1).wait_recv()
            total = keep_2[m][k, 1 - s] + recv_2[m][k, 1 - s].astype(jnp.float32)
            send_3[m][k] = total.astype(jnp.bfloat16)
            hop(piece, 2).start()
            keep_3[m][k] = keep_2[m][k, s] + recv_2[m][k, s].astype(jnp.float32)
        elif step == 3:
            if k == 0:
                for copy in params(m):
                    copy.wait()
            hop(piece, 2).wait_recv()
            at = pl.ds(k * rows, rows)
            mean = (keep_3[m][k] + recv_3[m][k].astype(jnp.float32)) * rate
            state = hold_rate * moment_v[m][at, :] + mean
            new = weight_v[m][at, :] - learn_rate * state
            own_v[m][k] = new.astype(jnp.bfloat16)
            hop(piece, 3).start()
            new_v[m][at, :] = new
            state_v[m][at, :] = state
            for copy in own_copies(piece):
                copy.start()
        elif step == 4:
            own_copies(piece)[0].wait()
            hop(piece, 3).wait_recv()
            hop(piece, 4).start()
        elif step == 5:
            hop(piece, 4).wait_recv()
            hop(piece, 5).start()
        else:
            hop(piece, 5).wait_recv()

    started = set()
    for p in range(pairs):
        for s in range(2):
            load(lists[s][p]).start()
        if p >= 1:
            for s in range(2):
                m = lists[s][p - 1][0]
                if m not in started:
                    started.add(m)
                    for copy in params(m):
                        copy.start()
    for m in range(6):
        if m not in started:
            for copy in params(m):
                copy.start()

    barrier = pltpu.get_barrier_semaphore()
    for d in range(1, n):
        pl.semaphore_signal(
            barrier, inc=1, device_id={"batch": lax.rem(me + d, n)}, device_id_type=pl.DeviceIdType.MESH
        )
    pl.semaphore_wait(barrier, n - 1)

    width = weight_norm.shape[1]

    def norm_hop(d):
        to = lax.rem(me + d, n)
        return pltpu.make_async_remote_copy(
            src_ref=norm_send.at[to],
            dst_ref=norm_recv.at[d],
            send_sem=norm_sems.at[0, d],
            recv_sem=norm_sems.at[1, d],
            device_id={"batch": to},
            device_id_type=pl.DeviceIdType.MESH,
        )

    def norm_back(d):
        to = lax.rem(me + d, n)
        return pltpu.make_async_remote_copy(
            src_ref=norm_pack.at[0],
            dst_ref=norm_all.at[d],
            send_sem=norm_sems_2.at[0, d],
            recv_sem=norm_sems_2.at[1, d],
            device_id={"batch": to},
            device_id_type=pl.DeviceIdType.MESH,
        )

    def norm_loads():
        return [
            pltpu.make_async_copy(source, target, norm_sems_3.at[i])
            for i, (source, target) in enumerate(zip(norm_inputs, norm_held))
        ]

    def norm_start():
        for copy in norm_loads():
            copy.wait()
        for j in range(n):
            part = grad_norm[:, j * width : (j + 1) * width]
            norm_send[j] = jnp.broadcast_to(part, (8, width))
        for d in range(1, n):
            norm_hop(d).start()

    def norm_update():
        total = norm_send[me]
        for d in range(1, n):
            norm_hop(d).wait_recv()
            total = total + norm_recv[d]
        state = hold_rate * moment_norm[...] + total * rate
        norm_pack[1] = state
        norm_pack[0] = weight_norm[...] - learn_rate * state
        for d in range(1, n):
            norm_back(d).start()

    def norm_end():
        norm_out[me] = norm_pack[0]
        for d in range(1, n):
            norm_back(d).wait_recv()
            norm_out[lax.rem(me + n - d, n)] = norm_all[d]

    for copy in norm_loads():
        copy.start()
    for slot in range(pairs + DELAYS[-1]):
        for step in STEP_ORDER:
            p = slot - DELAYS[step]
            if 0 <= p < pairs:
                for s in range(2):
                    stage(lists[s][p], step)
        if slot == 1:
            norm_start()
        if slot == 3:
            norm_update()
    norm_end()

    for p in range(pairs):
        for s in range(2):
            piece = lists[s][p]
            for step in range(6):
                hop(piece, step).wait_send()
            for copy in own_copies(piece)[1:]:
                copy.wait()
    for d in range(1, n):
        norm_hop(d).wait_send()
        norm_back(d).wait_send()


def write_out(shapes, n, *refs):
    refs = list(refs)

    def take(count):
        out, refs[:] = refs[:count], refs[count:]
        return out

    gathered, news, states = take(6), take(6), take(6)
    norm_pack, norm_out = take(2)
    copies, new_outs, state_outs = take(6), take(6), take(6)
    copy_norm, new_norm, state_norm = take(3)
    (sems,) = take(1)
    started = []
    count = 0
    for m in range(6):
        rows = shapes[m][0] // PIECES[m]
        width = shapes[m][1]
        for k in range(PIECES[m]):
            for j in range(n):
                source = gathered[m].at[k, j // 4, j // 2 % 2, j % 2]
                if BY_ROWS[m]:
                    target = copies[m].at[pl.ds(j * shapes[m][0] + k * rows, rows), :]
                else:
                    target = copies[m].at[pl.ds(k * rows, rows), pl.ds(j * width, width)]
                started.append(pltpu.make_async_copy(source, target, sems.at[count]))
                count += 1
        for source, target in ((news[m], new_outs[m]), (states[m], state_outs[m])):
            started.append(pltpu.make_async_copy(source, target, sems.at[count]))
            count += 1
    for copy in started:
        copy.start()
    for j in range(n):
        width = norm_out.shape[2]
        copy_norm[:, j * width : (j + 1) * width] = norm_out[j, 0:1, :].astype(jnp.bfloat16)
    new_norm[...] = norm_pack[0, 0:1, :]
    state_norm[...] = norm_pack[1, 0:1, :]
    for copy in started:
        copy.wait()


def kernel_body(*args):
    n = lax.axis_size("batch")
    grads, grad_norm = [a[0] for a in args[:6]], args[6]
    weights, weight_norm = args[7:13], args[13]
    moments, moment_norm = args[14:20], args[20]
    shapes = [w.shape for w in weights]
    grads = [g.reshape((n, *s)) if by_rows else g for g, s, by_rows in zip(grads, shapes, BY_ROWS)]
    width = weight_norm.shape[0]
    bf16, f32 = jnp.bfloat16, jnp.float32
    any_spec = pl.BlockSpec(memory_space=pl.ANY)
    vmem_spec = pl.BlockSpec(memory_space=pltpu.VMEM)
    hbm_spec = pl.BlockSpec(memory_space=pltpu.HBM)

    def cut(m):
        rows, cols = shapes[m]
        return PIECES[m], rows // PIECES[m], cols

    every = range(6)

    def scratch(lead, kind):
        return [pltpu.VMEM((cut(m)[0], *lead, *cut(m)[1:]), kind) for m in every]

    whole = [pltpu.VMEM(s, f32) for s in shapes]
    held = [pltpu.VMEM((cut(m)[0], 2, 2, 2, *cut(m)[1:]), bf16) for m in every] + whole + whole
    lists = pieces_of(shapes)
    assert len(lists[0]) == len(lists[1])
    norms = (grad_norm, weight_norm.reshape(1, width), moment_norm.reshape(1, width))
    arrays = (*grads, *weights, *moments, *norms)
    results = pl.pallas_call(
        functools.partial(exchange, shapes, n),
        out_shape=held
        + [jax.ShapeDtypeStruct((2, 8, width), f32), jax.ShapeDtypeStruct((n, 8, width), f32)],
        in_specs=[any_spec] * 21,
        out_specs=[any_spec] * 18 + [vmem_spec] * 2,
        scratch_shapes=[pltpu.VMEM(g.shape, f32) for g in grads]
        + whole * 4
        + scratch((4,), bf16) * 2
        + scratch((2,), bf16) * 2
        + scratch((2,), f32)
        + scratch((), bf16) * 2
        + scratch((), f32)
        + scratch((), bf16)
        + [pltpu.VMEM((n, 8, width), f32)] * 3
        + [pltpu.VMEM((1, n * width), f32)]
        + [pltpu.VMEM((1, width), f32)] * 2
        + [
            pltpu.SemaphoreType.DMA((2 * len(lists[0]), KINDS)),
            pltpu.SemaphoreType.DMA((6, 2)),
            pltpu.SemaphoreType.DMA((2, n)),
            pltpu.SemaphoreType.DMA((2, n)),
            pltpu.SemaphoreType.DMA((3,)),
        ],
        compiler_params=pltpu.CompilerParams(
            collective_id=0, has_side_effects=True, vmem_limit_bytes=40 * 2**20
        ),
    )(*[pltpu.with_memory_space_constraint(a, pltpu.HBM) for a in arrays])
    copies = n * sum(PIECES) + 12
    finals = pl.pallas_call(
        functools.partial(write_out, shapes, n),
        out_shape=[
            jax.ShapeDtypeStruct((n * s[0], s[1]) if by_rows else (s[0], n * s[1]), bf16)
            for s, by_rows in zip(shapes, BY_ROWS)
        ]
        + [jax.ShapeDtypeStruct(s, f32) for s in shapes] * 2
        + [
            jax.ShapeDtypeStruct((1, n * width), bf16),
            jax.ShapeDtypeStruct((1, width), f32),
            jax.ShapeDtypeStruct((1, width), f32),
        ],
        in_specs=[any_spec] * 18 + [vmem_spec] * 2,
        out_specs=[hbm_spec] * 18 + [vmem_spec] * 3,
        scratch_shapes=[pltpu.SemaphoreType.DMA((copies,))],
        compiler_params=pltpu.CompilerParams(vmem_limit_bytes=8 * 2**20),
    )(*[pltpu.with_memory_space_constraint(r, pltpu.VMEM) for r in results[:18]], *results[18:])
    copy, new, state = finals[:6], finals[6:12], finals[12:18]
    copy_norm, new_norm, state_norm = (r.reshape(r.shape[1]) for r in finals[18:])
    return (*copy, copy_norm, *new, new_norm, *state, state_norm)


def chosen(*args):
    fits = lax.axis_size("batch") == 2**3 and args[13].shape[0] % 128 == 0
    for w, count in zip(args[7:13], PIECES):
        fits = fits and w.shape[0] % (16 * count) == 0 and w.shape[1] % 128 == 0
    return kernel_body(*args) if fits else body(*args)


def solution(mesh):
    in_specs = (
        P("batch", None, "cols"),
        P("batch", "cols", None),
        P("batch", None, "cols"),
        P("batch", None, "cols"),
        P("batch", None, "cols"),
        P("batch", "cols", None),
        P("batch", None),
        P("batch", "cols"),
        P("cols", "batch"),
        P("batch", "cols"),
        P("batch", "cols"),
        P("batch", "cols"),
        P("cols", "batch"),
        P("batch"),
        P("batch", "cols"),
        P("cols", "batch"),
        P("batch", "cols"),
        P("batch", "cols"),
        P("batch", "cols"),
        P("cols", "batch"),
        P("batch"),
    )
    out_specs = (
        P(None, "cols"),
        P("cols", None),
        P(None, "cols"),
        P(None, "cols"),
        P(None, "cols"),
        P("cols", None),
        P(),
        P("batch", "cols"),
        P("cols", "batch"),
        P("batch", "cols"),
        P("batch", "cols"),
        P("batch", "cols"),
        P("cols", "batch"),
        P("batch"),
        P("batch", "cols"),
        P("cols", "batch"),
        P("batch", "cols"),
        P("batch", "cols"),
        P("batch", "cols"),
        P("cols", "batch"),
        P("batch"),
    )
    return jax.shard_map(chosen, mesh=mesh, in_specs=in_specs, out_specs=out_specs, check_vma=False)
```
